32 devices in a mesh: ep: 4 (over z), fsdp: 8 (over y, x, core).
Axes of the slice: x: 2, y: 2, z: 4, core: 2. Of those that a mesh axis runs over, the one named last changes fastest.
Arguments:
- train_gate: float32 [64, 2048, 1408], P('ep', 'fsdp'), may hold values from -0.1875 to 0.1875
- train_up: float32 [64, 2048, 1408], P('ep', 'fsdp'), may hold values from -0.1875 to 0.1875
- train_down: float32 [64, 1408, 2048], P('ep', None, 'fsdp'), may hold values from -0.21875 to 0.21875
- router_weight: float32 [2048, 64], P('fsdp', 'ep'), may hold values from -0.125 to 0.125
- router_gain: float32 [2048], P('fsdp'), may hold values from 0.25 to 1.75
Outputs:
- ready_gate: bfloat16 [64, 2048, 1408], P('ep', None, 'fsdp')
- ready_up: bfloat16 [64, 2048, 1408], P('ep', None, 'fsdp')
- ready_down: bfloat16 [64, 1408, 2048], P('ep', 'fsdp')
- scale_gate: float32 [64, 1408], P('ep', 'fsdp')
- scale_up: float32 [64, 1408], P('ep', 'fsdp')
- scale_down: float32 [64, 1408], P('ep', 'fsdp')
- serve_router: bfloat16 [2048, 64], replicated
The draws below stay inside these ranges and needn't reach their ends.
All inputs are finite; a program needn't handle non-finite values. Where the reference program divides by a largest or mean magnitude, that divisor is 1e-20 or more.
Results may differ from the reference program's by a relative error of at most 0.012.
Values may be sent and summed in bfloat16 or wider, within the bound.
A program may use at most 192 MiB of HBM per device.

```python
import jax
import jax.numpy as jnp

EXPERTS = 64
D_MODEL = 2048
D_EXPERT = 1408


def spiked(array, key, source, target, parts, factor):
    owner, partner = [(jnp.arange(array.shape[axis_at]) // (array.shape[axis_at] // parts)).reshape([-1 if axis == axis_at else 1 for axis in range(array.ndim)]) for axis_at in (source, target)]
    chosen = jax.random.permutation(key, parts)[partner]
    strong = (owner == chosen) | (owner == (partner + parts // 2) % parts)
    return jnp.where(strong, factor * array, array)


def block_levels(rng, extent, cuts, smallest, high):
    loudness = 1.0
    for axis_at, shards_of in cuts:
        heights = jax.random.uniform(jax.random.fold_in(jax.random.fold_in(rng, 6), axis_at), (shards_of,), jnp.float32, smallest / len(cuts), high / len(cuts))
        loudness = loudness * jnp.repeat(jnp.exp(heights), extent[axis_at] // shards_of).reshape((-1,) + (1,) * (len(extent) - 1 - axis_at))
    return loudness


def scatter_about(rng, shape, spread, reach, split=(), dtype=jnp.bfloat16):
    drawn = spread * jax.random.normal(rng, shape, jnp.float32)
    if split:
        drawn = drawn * block_levels(rng, shape, split, -0.22, 0.18)
    return jnp.clip(drawn, -reach, reach).astype(dtype)


def bell_draw_with(key, shape, spread, bound, pieces, heavy, dtype=jnp.bfloat16):
    array = spread * jax.random.normal(key, shape, jnp.float32)
    if pieces:
        array = array * block_levels(key, shape, pieces, -0.22, 0.18)
    return jnp.clip(spiked(array, jax.random.fold_in(key, 3), *heavy), -bound, bound).astype(dtype)


def setup_inputs(seed: int = 0) -> dict:
    splits = jax.random.split(jax.random.key(seed), 6)
    train_gate = bell_draw_with(splits[0], (EXPERTS, D_MODEL, D_EXPERT), D_MODEL ** -0.5, 0.1875, ((0, 4), (1, 8)), (1, 2, 8, 2.0), jnp.float32)
    train_up = bell_draw_with(splits[1], (EXPERTS, D_MODEL, D_EXPERT), D_MODEL ** -0.5, 0.1875, ((0, 4), (1, 8)), (1, 2, 8, 2.0), jnp.float32)
    train_down = bell_draw_with(splits[2], (EXPERTS, D_EXPERT, D_MODEL), D_EXPERT ** -0.5, 0.21875, ((0, 4), (2, 8)), (2, 1, 8, 2.0), jnp.float32)
    router_weight = scatter_about(splits[3], (D_MODEL, EXPERTS), D_MODEL ** -0.5, 0.125, ((0, 8), (1, 4)), jnp.float32)
    router_gain = jnp.clip(1.0 + 0.15 * jax.random.normal(splits[4], (D_MODEL,), jnp.float32), 0.25, 1.75)
    return {"train_gate": train_gate, "train_up": train_up, "train_down": train_down, "router_weight": router_weight, "router_gain": router_gain}


def reference(train_gate, train_up, train_down, router_weight, router_gain):
    scale_gate = jnp.sum(jnp.abs(train_gate), axis=1) / D_MODEL
    ready_gate = (train_gate / jnp.expand_dims(scale_gate, 1)).astype(jnp.bfloat16)
    scale_up = jnp.sum(jnp.abs(train_up), axis=1) / D_MODEL
    ready_up = (train_up / jnp.expand_dims(scale_up, 1)).astype(jnp.bfloat16)
    scale_down = jnp.sum(jnp.abs(train_down), axis=2) / D_MODEL
    ready_down = (train_down / jnp.expand_dims(scale_down, 2)).astype(jnp.bfloat16)
    serve_router = (router_weight * router_gain[:, None]).astype(jnp.bfloat16)
    return ready_gate, ready_up, ready_down, scale_gate, scale_up, scale_down, serve_router
```

```python
import functools

import jax
import jax.numpy as jnp
from jax import lax
from jax.experimental import pallas as pl
from jax.experimental.pallas import tpu as pltpu
from jax.sharding import PartitionSpec as P

VMEM_LIMIT = 60 * 1024 * 1024
FINISH_LIMIT = 24 * 1024 * 1024
TILE = 16
DEPTH = 4
MESH = pl.DeviceIdType.MESH
RING = 6


def ship_kernel(
    sizes, keep, down_ref, gate_ref, up_ref, router_ref, gain_ref,
    received_ref, packed_ref, copies_ref,
    down_in, gate_in, up_in, ring, column,
    load_sem, send_sem, recv_sem, router_sem,
):
    ep, fsdp = sizes
    row, me = lax.axis_index("ep"), lax.axis_index("fsdp")
    experts = down_ref.shape[0]
    sources = ((down_ref, down_in), (gate_ref, gate_in), (up_ref, up_in))

    def load(e, kind):
        source, held = sources[kind]
        slot = lax.rem(e, 2)
        return pltpu.make_async_copy(source.at[e], held.at[slot], load_sem.at[slot, kind])

    def pack(e, kind):
        block = sources[kind][1][lax.rem(e, 2)].astype(jnp.bfloat16)
        if kind:
            block = block.T
        ring[lax.rem(e, RING), kind] = block.reshape(ring.shape[2:])

    def sent(e, kind):
        at = ring.at[lax.rem(e, RING), kind]
        return pltpu.make_async_copy(at, received_ref.at[:, 0, kind], send_sem.at[lax.rem(e, RING), kind])

    def send(e, kind):
        slot = lax.rem(e, RING)
        for step in range(1, fsdp):
            peer = lax.rem(me + step, fsdp)
            pltpu.make_async_remote_copy(
                src_ref=ring.at[slot, kind, peer],
                dst_ref=received_ref.at[me, e, kind],
                send_sem=send_sem.at[slot, kind],
                recv_sem=recv_sem.at[e],
                device_id={"fsdp": peer},
                device_id_type=MESH,
            ).start()
        pltpu.make_async_copy(
            ring.at[slot, kind, me], received_ref.at[me, e, kind], send_sem.at[slot, kind]
        ).start()

    for e in range(min(2, experts)):
        for kind in range(3):
            load(e, kind).start()

    barrier = pltpu.get_barrier_semaphore()
    for step in range(1, fsdp):
        pl.semaphore_signal(barrier, device_id={"fsdp": lax.rem(me + step, fsdp)}, device_id_type=MESH)
    for step in range(1, ep):
        pl.semaphore_signal(barrier, device_id={"ep": lax.rem(row + step, ep)}, device_id_type=MESH)
    column[row] = (router_ref[...] * gain_ref[...]).astype(jnp.bfloat16)
    pl.semaphore_wait(barrier, fsdp + ep - 2)

    def step_of(e, carry):
        for kind in range(3):
            load(e, kind).wait()

            @pl.when(e >= RING)
            def _():
                sent(e - RING, kind).wait()

            pack(e, kind)

            @pl.when(e + 2 < experts)
            def _():
                load(e + 2, kind).start()

            @pl.when(e < keep)
            def _():
                send(e, kind)

            @pl.when(e >= keep)
            def _():
                slot = lax.rem(e, RING)
                pltpu.make_async_copy(
                    ring.at[slot, kind], packed_ref.at[:, e - keep, kind], send_sem.at[slot, kind]
                ).start()

        return carry

    first = min(RING, keep)
    lax.fori_loop(0, first, step_of, 0)

    def share_row(step):
        return pltpu.make_async_remote_copy(
            src_ref=column.at[row],
            dst_ref=column.at[row],
            send_sem=router_sem.at[0],
            recv_sem=router_sem.at[1],
            device_id={"ep": lax.rem(row + step, ep)},
            device_id_type=MESH,
        )

    def block_of(index):
        width = column.shape[2]
        return copies_ref.at[:, :, pl.ds(pl.multiple_of(index * width, width), width)]

    def share_column(step):
        return pltpu.make_async_remote_copy(
            src_ref=column,
            dst_ref=block_of(me),
            send_sem=router_sem.at[2],
            recv_sem=router_sem.at[3],
            device_id={"fsdp": lax.rem(me + step, fsdp)},
            device_id_type=MESH,
        )

    for step in range(1, ep):
        share_row(step).start()
    lax.fori_loop(first, experts, step_of, 0)
    rows = column.at[pl.ds(0, ep - 1)]
    pltpu.make_async_copy(rows, rows, router_sem.at[0]).wait()
    pltpu.make_async_copy(rows, rows, router_sem.at[1]).wait()
    for step in range(1, fsdp):
        share_column(step).start()
    own = pltpu.make_async_copy(column, block_of(me), router_sem.at[4])
    own.start()

    def settle(e, carry):
        for kind in range(3):
            sent(e, kind).wait()
        return carry

    lax.fori_loop(max(experts - RING, 0), experts, settle, 0)

    def arrive(e, carry):
        blocks = received_ref.at[pl.ds(0, fsdp - 1), e]
        pltpu.make_async_copy(blocks, blocks, recv_sem.at[e]).wait()
        return carry

    lax.fori_loop(0, keep, arrive, 0)
    width = column.shape[2]
    others = copies_ref.at[:, :, pl.ds(0, (fsdp - 1) * width)]
    pltpu.make_async_copy(others, others, router_sem.at[2]).wait()
    pltpu.make_async_copy(others, others, router_sem.at[3]).wait()
    own.wait()


def ship(ep, fsdp, keep, down, gate, up, router, gain):
    experts, rows, columns = gate.shape
    share = columns // fsdp
    last = experts - keep
    hbm = pl.BlockSpec(memory_space=pl.ANY)
    vmem = pl.BlockSpec(memory_space=pltpu.VMEM)
    return pl.pallas_call(
        functools.partial(ship_kernel, (ep, fsdp), keep),
        in_specs=[hbm, hbm, hbm, vmem, vmem],
        out_specs=[hbm, hbm, hbm],
        out_shape=[
            jax.ShapeDtypeStruct((fsdp, keep, 3, share, rows), jnp.bfloat16),
            jax.ShapeDtypeStruct((fsdp, last, 3, share, rows), jnp.bfloat16),
            jax.ShapeDtypeStruct((ep, router.shape[0], fsdp * router.shape[1]), jnp.bfloat16),
        ],
        scratch_shapes=[
            pltpu.VMEM((2, columns, rows), jnp.float32),
            pltpu.VMEM((2, rows, columns), jnp.float32),
            pltpu.VMEM((2, rows, columns), jnp.float32),
            pltpu.VMEM((RING, 3, fsdp, share, rows), jnp.bfloat16),
            pltpu.VMEM((ep,) + router.shape, jnp.bfloat16),
            pltpu.SemaphoreType.DMA((2, 3)),
            pltpu.SemaphoreType.DMA((RING, 3)),
            pltpu.SemaphoreType.DMA((keep,)),
            pltpu.SemaphoreType.DMA((5,)),
        ],
        compiler_params=pltpu.CompilerParams(
            collective_id=0, has_side_effects=True, vmem_limit_bytes=VMEM_LIMIT
        ),
        cost_estimate=pl.CostEstimate(
            flops=experts * rows * columns * 30, bytes_accessed=experts * rows * columns * 18, transcendentals=0
        ),
    )(down, gate, up, router, gain)


def rescale(blocks, width, ready, scale_ref, e):
    peers, share, inner = blocks.shape
    columns = []
    for r in range(0, share, TILE):
        rows = slice(r, min(r + TILE, share))
        parts = [blocks[p, rows].astype(jnp.float32) for p in range(peers)]
        total = sum(jnp.abs(part) for part in parts)
        scale = jnp.sum(total, axis=1, keepdims=True) / width
        inverse = 1.0 / scale
        for p, part in enumerate(parts):
            ready[rows, p * inner : (p + 1) * inner] = (part * inverse).astype(jnp.bfloat16)
        columns.append(scale)
    column = jnp.concatenate(columns, axis=0)
    scale_ref[pl.ds(e, 1), :] = jnp.broadcast_to(column, (share, 128)).T[0:1]


def finish_kernel(x_ref, copies_ref, *refs):
    readies, scales, router_ref = refs[:3], refs[3:6], refs[6]
    held, ready, router, load_sem, store_sem, router_sem = refs[7:]
    peers, count, _, share, inner = x_ref.shape

    def load(e):
        slot = lax.rem(e, DEPTH)
        return pltpu.make_async_copy(x_ref.at[:, e], held.at[slot], load_sem.at[slot])

    def store(e, kind):
        slot = lax.rem(e, DEPTH)
        return pltpu.make_async_copy(ready.at[slot, kind], readies[kind].at[e], store_sem.at[slot, kind])

    for e in range(min(DEPTH, count)):
        load(e).start()
    enter = pltpu.make_async_copy(copies_ref, router, router_sem.at[0])
    leave = pltpu.make_async_copy(router, router_ref, router_sem.at[1])
    enter.start()

    def step_of(e, carry):
        slot = lax.rem(e, DEPTH)
        load(e).wait()
        for kind in range(3):

            @pl.when(e >= DEPTH)
            def _():
                store(e - DEPTH, kind).wait()

            rescale(held.at[slot, :, kind], peers * inner, ready.at[slot, kind], scales[kind], e)
            store(e, kind).start()

        @pl.when(e + DEPTH < count)
        def _():
            load(e + DEPTH).start()

        return carry

    lax.fori_loop(0, count, step_of, 0)
    enter.wait()
    leave.start()

    def settle(e, carry):
        for kind in range(3):
            store(e, kind).wait()
        return carry

    lax.fori_loop(max(count - DEPTH, 0), count, settle, 0)
    leave.wait()


def finish(received, copies, experts):
    peers, count, _, share, inner = received.shape
    width = peers * inner
    hbm = pl.BlockSpec(memory_space=pl.ANY)
    vmem = pl.BlockSpec(memory_space=pltpu.VMEM)
    return pl.pallas_call(
        finish_kernel,
        in_specs=[hbm, hbm],
        out_specs=[hbm] * 3 + [vmem] * 3 + [hbm],
        out_shape=[jax.ShapeDtypeStruct((experts, share, width), jnp.bfloat16)] * 3
        + [jax.ShapeDtypeStruct((experts, share), jnp.float32)] * 3
        + [jax.ShapeDtypeStruct(copies.shape, jnp.bfloat16)],
        scratch_shapes=[
            pltpu.VMEM((DEPTH, peers, 3, share, inner), jnp.bfloat16),
            pltpu.VMEM((DEPTH, 3, share, width), jnp.bfloat16),
            pltpu.VMEM(copies.shape, jnp.bfloat16),
            pltpu.SemaphoreType.DMA((DEPTH,)),
            pltpu.SemaphoreType.DMA((DEPTH, 3)),
            pltpu.SemaphoreType.DMA((2,)),
        ],
        compiler_params=pltpu.CompilerParams(vmem_limit_bytes=VMEM_LIMIT - 8 * 1024 * 1024),
        cost_estimate=pl.CostEstimate(
            flops=count * share * width * 12, bytes_accessed=count * share * width * 12, transcendentals=0
        ),
    )(received, copies)


def close_kernel(first, x_ref, *refs):
    before, readies, scales = refs[3:6], refs[6:9], refs[9:12]
    ready, store_sem = refs[12:]
    peers, count, _, share, inner = x_ref.shape
    for old, new in zip(before, scales):
        new[...] = old[...]
    stores = []
    for e in range(count):
        for kind in range(3):
            rescale(x_ref.at[:, e, kind], peers * inner, ready.at[e, kind], scales[kind], first + e)
            store = pltpu.make_async_copy(ready.at[e, kind], readies[kind].at[first + e], store_sem.at[e, kind])
            store.start()
            stores.append(store)
    for store in stores:
        store.wait()


def close(received, first, carried):
    peers, count, _, share, inner = received.shape
    width = peers * inner
    hbm = pl.BlockSpec(memory_space=pl.ANY)
    vmem = pl.BlockSpec(memory_space=pltpu.VMEM)
    return pl.pallas_call(
        functools.partial(close_kernel, first),
        in_specs=[vmem] + [hbm] * 3 + [vmem] * 3,
        out_specs=[hbm] * 3 + [vmem] * 3,
        out_shape=[jax.ShapeDtypeStruct(old.shape, old.dtype) for old in carried],
        input_output_aliases={1: 0, 2: 1, 3: 2},
        scratch_shapes=[
            pltpu.VMEM((count, 3, share, width), jnp.bfloat16),
            pltpu.SemaphoreType.DMA((count, 3)),
        ],
        compiler_params=pltpu.CompilerParams(vmem_limit_bytes=FINISH_LIMIT),
        cost_estimate=pl.CostEstimate(
            flops=count * share * width * 12, bytes_accessed=count * share * width * 12, transcendentals=0
        ),
    )(received, *carried)


def shards(ep, fsdp, train_gate, train_up, train_down, router_weight, router_gain):
    experts = train_gate.shape[0]
    last = max(experts // 16, 1)
    keep = experts - last
    received, packed, copies = ship(
        ep, fsdp, keep, train_down, train_gate, train_up, router_weight.T, router_gain[None]
    )
    rest = lax.all_to_all(packed, "fsdp", split_axis=0, concat_axis=0, tiled=True)
    *done, copies = finish(received, copies, experts)
    ready_down, ready_gate, ready_up, scale_down, scale_gate, scale_up = close(rest, keep, done)
    serve_router = copies.reshape(-1, copies.shape[2]).T
    return (
        jnp.swapaxes(ready_gate, 1, 2),
        jnp.swapaxes(ready_up, 1, 2),
        ready_down,
        scale_gate,
        scale_up,
        scale_down,
        serve_router,
    )


def solution(mesh):
    in_specs = (
        P("ep", "fsdp", None),
        P("ep", "fsdp", None),
        P("ep", None, "fsdp"),
        P("fsdp", "ep"),
        P("fsdp"),
    )
    out_specs = (
        P("ep", None, "fsdp"),
        P("ep", None, "fsdp"),
        P("ep", "fsdp", None),
        P("ep", "fsdp"),
        P("ep", "fsdp"),
        P("ep", "fsdp"),
        P(),
    )
    body = functools.partial(shards, mesh.shape["ep"], mesh.shape["fsdp"])
    return jax.shard_map(body, mesh=mesh, in_specs=in_specs, out_specs=out_specs, check_vma=False)
```

```python
import functools

import jax
import jax.numpy as jnp
from jax import lax
from jax.experimental import pallas as pl
from jax.experimental.pallas import tpu as pltpu
from jax.sharding import PartitionSpec as P

VMEM_LIMIT = 60 * 1024 * 1024
FINISH_LIMIT = 24 * 1024 * 1024
TILE = 16
DEPTH = 6
MESH = pl.DeviceIdType.MESH
RING = 6


def ship_kernel(
    sizes, keep, down_ref, gate_ref, up_ref, router_ref, gain_ref,
    received_ref, packed_ref, copies_ref,
    down_in, gate_in, up_in, ring, weight, gain, strip,
    load_sem, send_sem, recv_sem, piece_sem, router_sem,
):
    ep, fsdp = sizes
    row, me = lax.axis_index("ep"), lax.axis_index("fsdp")
    experts = down_ref.shape[0]
    sources = ((down_ref, down_in), (gate_ref, gate_in), (up_ref, up_in))

    def load(e, kind):
        source, held = sources[kind]
        slot = lax.rem(e, 2)
        return pltpu.make_async_copy(source.at[e], held.at[slot], load_sem.at[slot, kind])

    def pack(e, kind):
        block = sources[kind][1][lax.rem(e, 2)].astype(jnp.bfloat16)
        if kind:
            block = block.T
        ring[lax.rem(e, RING), :, kind] = block.reshape(fsdp, *ring.shape[3:])

    def sent(e):
        slot = lax.rem(e, RING)
        return pltpu.make_async_copy(ring.at[slot], received_ref.at[:, 0], send_sem.at[slot])

    order = [lax.rem(me + step, fsdp) for step in range(1, fsdp + 1)]

    def ship(src, dst, slot, e, peer):
        return pltpu.make_async_remote_copy(
            src_ref=src,
            dst_ref=dst,
            send_sem=send_sem.at[slot],
            recv_sem=recv_sem.at[e],
            device_id={"fsdp": peer},
            device_id_type=MESH,
        )

    def send(e):
        slot = lax.rem(e, RING)
        for peer in order[:-1]:
            ship(ring.at[slot, peer], received_ref.at[me, e], slot, e, peer).start()
        pltpu.make_async_copy(ring.at[slot, me], received_ref.at[me, e], send_sem.at[slot]).start()

    def piece(at, p):
        share = ring.shape[3]
        rows = pl.ds(pl.multiple_of(p * share, share), share)
        return pltpu.make_async_copy(down_ref.at[0, rows], down_in.at[0, rows], piece_sem.at[at])

    for at, p in enumerate(order):
        piece(at, p).start()
    router = [
        pltpu.make_async_copy(src, dst, router_sem.at[at])
        for at, (src, dst) in enumerate(((router_ref, weight), (gain_ref, gain)))
    ]
    for kind in (1, 2):
        load(0, kind).start()
    for copy in router:
        copy.start()
    for kind in range(3):
        load(1, kind).start()

    barrier = pltpu.get_barrier_semaphore()
    for step in range(1, fsdp):
        pl.semaphore_signal(barrier, device_id={"fsdp": lax.rem(me + step, fsdp)}, device_id_type=MESH)
    for step in range(1, ep):
        pl.semaphore_signal(barrier, device_id={"ep": lax.rem(row + step, ep)}, device_id_type=MESH)
    pl.semaphore_wait(barrier, fsdp + ep - 2)

    for at, p in enumerate(order):
        piece(at, p).wait()
        share = ring.shape[3]
        rows = pl.ds(pl.multiple_of(p * share, share), share)
        ring[0, p, 0] = down_in[0, rows].astype(jnp.bfloat16)
        if at < fsdp - 1:
            ship(ring.at[0, p, 0], received_ref.at[me, 0, 0], 0, 0, p).start()
    for kind in (1, 2):
        load(0, kind).wait()
        pack(0, kind)
        for peer in order[:-1]:
            ship(ring.at[0, peer, kind], received_ref.at[me, 0, kind], 0, 0, peer).start()
    pltpu.make_async_copy(ring.at[0, me], received_ref.at[me, 0], send_sem.at[0]).start()
    if experts > 2:
        for kind in range(3):
            load(2, kind).start()

    def step_of(e, carry):
        for kind in range(3):
            load(e, kind).wait()
            if kind == 0:

                @pl.when(e >= RING)
                def _():
                    sent(e - RING).wait()

            pack(e, kind)

            @pl.when(e + 2 < experts)
            def _():
                load(e + 2, kind).start()

        @pl.when(e < keep)
        def _():
            send(e)

        @pl.when(e >= keep)
        def _():
            slot = lax.rem(e, RING)
            pltpu.make_async_copy(ring.at[slot], packed_ref.at[:, e - keep], send_sem.at[slot]).start()

        return carry

    first = min(RING, keep)
    lax.fori_loop(1, first, step_of, 0)

    width = weight.shape[1]
    mine = strip.at[:, pl.ds(pl.multiple_of(me * width, width), width)]
    for copy in router:
        copy.wait()
    mine[...] = (weight[...] * gain[...]).astype(jnp.bfloat16)
    for peer in order[:-1]:
        pltpu.make_async_remote_copy(
            src_ref=mine,
            dst_ref=mine,
            send_sem=router_sem.at[2],
            recv_sem=router_sem.at[3],
            device_id={"fsdp": peer},
            device_id_type=MESH,
        ).start()
    lax.fori_loop(first, keep, step_of, 0)
    others = strip.at[:, pl.ds(0, (fsdp - 1) * width)]
    pltpu.make_async_copy(others, others, router_sem.at[2]).wait()
    pltpu.make_async_copy(others, others, router_sem.at[3]).wait()
    for step in range(1, ep):
        pltpu.make_async_remote_copy(
            src_ref=strip,
            dst_ref=copies_ref.at[row],
            send_sem=router_sem.at[4],
            recv_sem=router_sem.at[5],
            device_id={"ep": lax.rem(row + step, ep)},
            device_id_type=MESH,
        ).start()
    own = pltpu.make_async_copy(strip, copies_ref.at[row], router_sem.at[6])
    own.start()
    lax.fori_loop(keep, experts, step_of, 0)

    def settle(e, carry):
        sent(e).wait()
        return carry

    lax.fori_loop(max(experts - RING, 0), experts, settle, 0)

    def arrive(e, carry):
        blocks = received_ref.at[pl.ds(0, fsdp - 1), e]
        pltpu.make_async_copy(blocks, blocks, recv_sem.at[e]).wait()
        return carry

    lax.fori_loop(0, keep, arrive, 0)
    others = copies_ref.at[pl.ds(0, ep - 1)]
    pltpu.make_async_copy(others, others, router_sem.at[4]).wait()
    pltpu.make_async_copy(others, others, router_sem.at[5]).wait()
    own.wait()


def ship(ep, fsdp, keep, down, gate, up, router, gain):
    experts, rows, columns = gate.shape
    share = columns // fsdp
    last = experts - keep
    hbm = pl.BlockSpec(memory_space=pl.ANY)
    return pl.pallas_call(
        functools.partial(ship_kernel, (ep, fsdp), keep),
        in_specs=[hbm] * 5,
        out_specs=[hbm, hbm, hbm],
        out_shape=[
            jax.ShapeDtypeStruct((fsdp, keep, 3, share, rows), jnp.bfloat16),
            jax.ShapeDtypeStruct((fsdp, last, 3, share, rows), jnp.bfloat16),
            jax.ShapeDtypeStruct((ep, router.shape[0], fsdp * router.shape[1]), jnp.bfloat16),
        ],
        scratch_shapes=[
            pltpu.VMEM((2, columns, rows), jnp.float32),
            pltpu.VMEM((2, rows, columns), jnp.float32),
            pltpu.VMEM((2, rows, columns), jnp.float32),
            pltpu.VMEM((RING, fsdp, 3, share, rows), jnp.bfloat16),
            pltpu.VMEM(router.shape, jnp.float32),
            pltpu.VMEM(gain.shape, jnp.float32),
            pltpu.VMEM((router.shape[0], fsdp * router.shape[1]), jnp.bfloat16),
            pltpu.SemaphoreType.DMA((2, 3)),
            pltpu.SemaphoreType.DMA((RING,)),
            pltpu.SemaphoreType.DMA((keep,)),
            pltpu.SemaphoreType.DMA((fsdp,)),
            pltpu.SemaphoreType.DMA((7,)),
        ],
        compiler_params=pltpu.CompilerParams(
            collective_id=0, has_side_effects=True, vmem_limit_bytes=VMEM_LIMIT
        ),
        cost_estimate=pl.CostEstimate(
            flops=experts * rows * columns * 30, bytes_accessed=experts * rows * columns * 18, transcendentals=0
        ),
    )(down, gate, up, router, gain)


def rescale(blocks, width, ready):
    peers, share, inner = blocks.shape
    columns = []
    for r in range(0, share, TILE):
        rows = slice(r, min(r + TILE, share))
        parts = [blocks[p, rows].astype(jnp.float32) for p in range(peers)]
        total = sum(jnp.abs(part) for part in parts)
        scale = jnp.sum(total, axis=1, keepdims=True) / width
        inverse = 1.0 / scale
        for p, part in enumerate(parts):
            ready[rows, p * inner : (p + 1) * inner] = (part * inverse).astype(jnp.bfloat16)
        columns.append(scale)
    column = jnp.concatenate(columns, axis=0)
    return jnp.broadcast_to(column, (share, 128)).T[0:1]


def finish_kernel(x_ref, copies_ref, *refs):
    readies, scales, router_ref = refs[:3], refs[3:6], refs[6]
    held, ready, router, load_sem, store_sem, router_sem = refs[7:]
    peers, count, _, share, inner = x_ref.shape

    def load(e, kind):
        slot = lax.rem(e, DEPTH)
        return pltpu.make_async_copy(x_ref.at[:, e, kind], held.at[slot, kind], load_sem.at[slot, kind])

    def store(e, kind):
        slot = lax.rem(e, DEPTH)
        return pltpu.make_async_copy(ready.at[slot, kind], readies[kind].at[e], store_sem.at[slot, kind])

    for e in range(min(DEPTH, count)):
        for kind in range(3):
            load(e, kind).start()
    enter = pltpu.make_async_copy(copies_ref, router, router_sem.at[0])
    leave = pltpu.make_async_copy(router, router_ref, router_sem.at[1])
    enter.start()

    def step_of(e, carry):
        slot = lax.rem(e, DEPTH)
        for kind in range(3):
            load(e, kind).wait()

            @pl.when(e >= DEPTH)
            def _():
                store(e - DEPTH, kind).wait()

            line = rescale(held.at[slot, kind], peers * inner, ready.at[slot, kind])
            scales[kind][pl.ds(e, 1), :] = line
            store(e, kind).start()

            @pl.when(e + DEPTH < count)
            def _():
                load(e + DEPTH, kind).start()

        return carry

    lax.fori_loop(0, count, step_of, 0)
    enter.wait()
    leave.start()

    def settle(e, carry):
        for kind in range(3):
            store(e, kind).wait()
        return carry

    lax.fori_loop(max(count - DEPTH, 0), count, settle, 0)
    leave.wait()


def finish(received, copies, experts):
    peers, count, _, share, inner = received.shape
    width = peers * inner
    hbm = pl.BlockSpec(memory_space=pl.ANY)
    vmem = pl.BlockSpec(memory_space=pltpu.VMEM)
    return pl.pallas_call(
        finish_kernel,
        in_specs=[hbm, hbm],
        out_specs=[hbm] * 3 + [vmem] * 3 + [hbm],
        out_shape=[jax.ShapeDtypeStruct((experts, share, width), jnp.bfloat16)] * 3
        + [jax.ShapeDtypeStruct((experts, share), jnp.float32)] * 3
        + [jax.ShapeDtypeStruct(copies.shape, jnp.bfloat16)],
        scratch_shapes=[
            pltpu.VMEM((DEPTH, 3, peers, share, inner), jnp.bfloat16),
            pltpu.VMEM((DEPTH, 3, share, width), jnp.bfloat16),
            pltpu.VMEM(copies.shape, jnp.bfloat16),
            pltpu.SemaphoreType.DMA((DEPTH, 3)),
            pltpu.SemaphoreType.DMA((DEPTH, 3)),
            pltpu.SemaphoreType.DMA((2,)),
        ],
        compiler_params=pltpu.CompilerParams(vmem_limit_bytes=VMEM_LIMIT),
        cost_estimate=pl.CostEstimate(
            flops=count * share * width * 12, bytes_accessed=count * share * width * 12, transcendentals=0
        ),
    )(received, copies)


def close_kernel(first, x_ref, *refs):
    readies, scales = refs[6:9], refs[9:12]
    ready, held, load_sem, store_sem = refs[12:]
    peers, count, _, share, inner = x_ref.shape
    loads = [pltpu.make_async_copy(scales[kind], held.at[kind], load_sem.at[kind]) for kind in range(3)]
    for load in loads:
        load.start()
    stores = []

    def store(src, dst):
        stores.append(pltpu.make_async_copy(src, dst, store_sem.at[len(stores)]))
        stores[-1].start()

    for kind in range(3):
        for e in range(count):
            line = rescale(x_ref.at[:, e, kind], peers * inner, ready.at[e, kind])
            store(ready.at[e, kind], readies[kind].at[first + e])
            if e == 0:
                loads[kind].wait()
            held[kind, first + e : first + e + 1, :] = line
        store(held.at[kind], scales[kind])
    for each in stores:
        each.wait()


def close(received, first, carried):
    peers, count, _, share, inner = received.shape
    width = peers * inner
    hbm = pl.BlockSpec(memory_space=pl.ANY)
    vmem = pl.BlockSpec(memory_space=pltpu.VMEM)
    return pl.pallas_call(
        functools.partial(close_kernel, first),
        in_specs=[vmem] + [hbm] * 6,
        out_specs=[hbm] * 6,
        out_shape=[jax.ShapeDtypeStruct(old.shape, old.dtype) for old in carried],
        input_output_aliases={at + 1: at for at in range(6)},
        scratch_shapes=[
            pltpu.VMEM((count, 3, share, width), jnp.bfloat16),
            pltpu.VMEM((3,) + carried[3].shape, jnp.float32),
            pltpu.SemaphoreType.DMA((3,)),
            pltpu.SemaphoreType.DMA((3 * count + 3,)),
        ],
        compiler_params=pltpu.CompilerParams(vmem_limit_bytes=FINISH_LIMIT),
        cost_estimate=pl.CostEstimate(
            flops=count * share * width * 12, bytes_accessed=count * share * width * 12, transcendentals=0
        ),
    )(received, *carried)


def shards(ep, fsdp, train_gate, train_up, train_down, router_weight, router_gain):
    experts = train_gate.shape[0]
    last = max(experts // 16, 1)
    keep = experts - last
    received, packed, copies = ship(
        ep, fsdp, keep, train_down, train_gate, train_up, router_weight.T, router_gain[None]
    )
    rest = lax.all_to_all(packed, "fsdp", split_axis=0, concat_axis=0, tiled=True)
    *done, copies = finish(received, copies, experts)
    ready_down, ready_gate, ready_up, scale_down, scale_gate, scale_up = close(rest, keep, done)
    serve_router = copies.reshape(-1, copies.shape[2]).T
    return (
        jnp.swapaxes(ready_gate, 1, 2),
        jnp.swapaxes(ready_up, 1, 2),
        ready_down,
        scale_gate,
        scale_up,
        scale_down,
        serve_router,
    )


def solution(mesh):
    in_specs = (
        P("ep", "fsdp", None),
        P("ep", "fsdp", None),
        P("ep", None, "fsdp"),
        P("fsdp", "ep"),
        P("fsdp"),
    )
    out_specs = (
        P("ep", None, "fsdp"),
        P("ep", None, "fsdp"),
        P("ep", "fsdp", None),
        P("ep", "fsdp"),
        P("ep", "fsdp"),
        P("ep", "fsdp"),
        P(),
    )
    body = functools.partial(shards, mesh.shape["ep"], mesh.shape["fsdp"])
    return jax.shard_map(body, mesh=mesh, in_specs=in_specs, out_specs=out_specs, check_vma=False)
```

```python
import functools

import jax
import jax.numpy as jnp
from jax import lax
from jax.experimental import pallas as pl
from jax.experimental.pallas import tpu as pltpu
from jax.sharding import PartitionSpec as P

VMEM_LIMIT = 60 * 1024 * 1024
FINISH_LIMIT = 24 * 1024 * 1024
TILE = 16
DEPTH = 6
MESH = pl.DeviceIdType.MESH
RING = 6


def turn(at, index, size, back=False):
    if size & (size - 1):
        return (index + (size - at if back else at)) % size
    bits = [1 << bit for bit in range(size.bit_length() - 1)]
    return sum(((index // bit + at // bit) % 2) * bit for bit in bits)


def wrap(e, size):
    return e % size if isinstance(e, int) else lax.rem(e, size)


def late_turns(fsdp):
    near = [at for at in range(2, fsdp) if bin(at // 2).count("1") == 1]
    return near + [at for at in range(2, fsdp) if at not in near]


def ship_kernel(sizes, keep, down_ref, gate_ref, up_ref, router_ref, gain_ref, received_ref, late_ref, copies_ref, *refs):
    ep, fsdp = sizes
    packed = dict(zip(late_turns(fsdp), refs))
    down_in, gate_in, up_in, ring, weight, gain, strip = refs[len(packed) : len(packed) + 7]
    load_sem, send_sem, recv_sem, piece_sem, router_sem = refs[len(packed) + 7 :]
    row, me = lax.axis_index("ep"), lax.axis_index("fsdp")
    experts = down_ref.shape[0]
    sources = ((down_ref, down_in), (gate_ref, gate_in), (up_ref, up_in))

    def load(e, kind):
        source, held = sources[kind]
        slot = wrap(e, 2)
        return pltpu.make_async_copy(source.at[e], held.at[slot], load_sem.at[slot, kind])

    def pack(e, kind):
        block = sources[kind][1][wrap(e, 2)].astype(jnp.bfloat16)
        if kind:
            block = block.T
        ring[wrap(e, RING), :, kind] = block.reshape(fsdp, *ring.shape[3:])

    def sent(e):
        slot = wrap(e, RING)
        return pltpu.make_async_copy(ring.at[slot], received_ref.at[:, 0], send_sem.at[slot])

    order = [lax.rem(me + step, fsdp) for step in range(1, fsdp + 1)]

    def ship(src, dst, slot, e, peer):
        return pltpu.make_async_remote_copy(
            src_ref=src,
            dst_ref=dst,
            send_sem=send_sem.at[slot],
            recv_sem=recv_sem.at[e],
            device_id={"fsdp": peer},
            device_id_type=MESH,
        )

    def send(e):
        slot = wrap(e, RING)
        for peer in order[:-1]:
            ship(ring.at[slot, peer], received_ref.at[me, e], slot, e, peer).start()
        pltpu.make_async_copy(ring.at[slot, me], received_ref.at[me, e], send_sem.at[slot]).start()

    def piece(at, p):
        share = ring.shape[3]
        rows = pl.ds(pl.multiple_of(p * share, share), share)
        return pltpu.make_async_copy(down_ref.at[0, rows], down_in.at[0, rows], piece_sem.at[at])

    for at, p in enumerate(order):
        piece(at, p).start()
    router = [
        pltpu.make_async_copy(src, dst, router_sem.at[at])
        for at, (src, dst) in enumerate(((router_ref, weight), (gain_ref, gain)))
    ]
    for kind in (1, 2):
        load(0, kind).start()
    for copy in router:
        copy.start()
    for kind in range(3):
        load(1, kind).start()

    barrier = pltpu.get_barrier_semaphore()
    for step in range(1, fsdp):
        pl.semaphore_signal(barrier, device_id={"fsdp": lax.rem(me + step, fsdp)}, device_id_type=MESH)
    for step in range(1, ep):
        pl.semaphore_signal(barrier, device_id={"ep": lax.rem(row + step, ep)}, device_id_type=MESH)
    pl.semaphore_wait(barrier, fsdp + ep - 2)

    for at, p in enumerate(order):
        piece(at, p).wait()
        share = ring.shape[3]
        rows = pl.ds(pl.multiple_of(p * share, share), share)
        ring[0, p, 0] = down_in[0, rows].astype(jnp.bfloat16)
        if at < fsdp - 1:
            ship(ring.at[0, p, 0], received_ref.at[me, 0, 0], 0, 0, p).start()
    for kind in (1, 2):
        load(0, kind).wait()
        pack(0, kind)
        for peer in order[:-1]:
            ship(ring.at[0, peer, kind], received_ref.at[me, 0, kind], 0, 0, peer).start()
    pltpu.make_async_copy(ring.at[0, me], received_ref.at[me, 0], send_sem.at[0]).start()
    if experts > 2:
        for kind in range(3):
            load(2, kind).start()

    def prepare(e, kind):
        load(e, kind).wait()
        if kind == 0:

            @pl.when(e >= RING)
            def _():
                sent(e - RING).wait()

        pack(e, kind)

        @pl.when(e + 2 < experts)
        def _():
            load(e + 2, kind).start()

    def step_of(e, carry):
        for kind in range(3):
            prepare(e, kind)
        send(e)
        return carry

    def set_by(e, kind, item):
        slot = e % RING
        for at, ref in packed.items():
            peer = turn(at, me, fsdp)
            pltpu.make_async_copy(ring.at[slot, peer, kind], ref.at[item], send_sem.at[slot]).start()
        peer = turn(1, me, fsdp)
        ship(ring.at[slot, peer, kind], late_ref.at[1, item], slot, keep, peer).start()
        pltpu.make_async_copy(ring.at[slot, me, kind], late_ref.at[0, item], send_sem.at[slot]).start()

    first = min(RING, keep - 1)
    lax.fori_loop(1, first, step_of, 0)

    width = weight.shape[1]
    mine = strip.at[:, pl.ds(pl.multiple_of(me * width, width), width)]
    for copy in router:
        copy.wait()
    mine[...] = (weight[...] * gain[...]).astype(jnp.bfloat16)
    for peer in order[:-1]:
        pltpu.make_async_remote_copy(
            src_ref=mine,
            dst_ref=mine,
            send_sem=router_sem.at[2],
            recv_sem=router_sem.at[3],
            device_id={"fsdp": peer},
            device_id_type=MESH,
        ).start()
    lax.fori_loop(first, keep - 1, step_of, 0)
    e, slot = keep - 1, (keep - 1) % RING
    prepare(e, 0)
    prepare(e, 1)
    two = pl.ds(0, 2)
    for peer in order[:-1]:
        ship(ring.at[slot, peer, two], received_ref.at[me, e, two], slot, e, peer).start()
    pltpu.make_async_copy(ring.at[slot, me, two], received_ref.at[me, e, two], send_sem.at[slot]).start()
    prepare(e, 2)
    set_by(e, 2, 0)
    others = strip.at[:, pl.ds(0, (fsdp - 1) * width)]
    pltpu.make_async_copy(others, others, router_sem.at[2]).wait()
    pltpu.make_async_copy(others, others, router_sem.at[3]).wait()
    for step in range(1, ep):
        pltpu.make_async_remote_copy(
            src_ref=strip,
            dst_ref=copies_ref.at[row],
            send_sem=router_sem.at[4],
            recv_sem=router_sem.at[5],
            device_id={"ep": lax.rem(row + step, ep)},
            device_id_type=MESH,
        ).start()
    own = pltpu.make_async_copy(strip, copies_ref.at[row], router_sem.at[6])
    own.start()
    for e in range(keep, experts):
        for kind in range(3):
            prepare(e, kind)
            set_by(e, kind, 1 + 3 * (e - keep) + kind)

    def settle(e, carry):
        sent(e).wait()
        return carry

    lax.fori_loop(max(experts - RING, 0), experts, settle, 0)

    def arrive(e, carry):
        blocks = received_ref.at[pl.ds(0, fsdp - 1), e]
        pltpu.make_async_copy(blocks, blocks, recv_sem.at[e]).wait()
        return carry

    lax.fori_loop(0, keep - 1, arrive, 0)
    blocks = received_ref.at[pl.ds(0, fsdp - 1), 0, two]
    pltpu.make_async_copy(blocks, blocks, recv_sem.at[keep - 1]).wait()
    pltpu.make_async_copy(late_ref.at[1], late_ref.at[1], recv_sem.at[keep]).wait()
    others = copies_ref.at[pl.ds(0, ep - 1)]
    pltpu.make_async_copy(others, others, router_sem.at[4]).wait()
    pltpu.make_async_copy(others, others, router_sem.at[5]).wait()
    own.wait()


def ship(ep, fsdp, keep, down, gate, up, router, gain):
    experts, rows, columns = gate.shape
    share = columns // fsdp
    late = 1 + 3 * (experts - keep)
    hbm = pl.BlockSpec(memory_space=pl.ANY)
    return pl.pallas_call(
        functools.partial(ship_kernel, (ep, fsdp), keep),
        in_specs=[hbm] * 5,
        out_specs=[hbm] * (fsdp + 1),
        out_shape=[
            jax.ShapeDtypeStruct((fsdp, keep, 3, share, rows), jnp.bfloat16),
            jax.ShapeDtypeStruct((2, late, share, rows), jnp.bfloat16),
            jax.ShapeDtypeStruct((ep, router.shape[0], fsdp * router.shape[1]), jnp.bfloat16),
        ]
        + [jax.ShapeDtypeStruct((late, share, rows), jnp.bfloat16)] * (fsdp - 2),
        scratch_shapes=[
            pltpu.VMEM((2, columns, rows), jnp.float32),
            pltpu.VMEM((2, rows, columns), jnp.float32),
            pltpu.VMEM((2, rows, columns), jnp.float32),
            pltpu.VMEM((RING, fsdp, 3, share, rows), jnp.bfloat16),
            pltpu.VMEM(router.shape, jnp.float32),
            pltpu.VMEM(gain.shape, jnp.float32),
            pltpu.VMEM((router.shape[0], fsdp * router.shape[1]), jnp.bfloat16),
            pltpu.SemaphoreType.DMA((2, 3)),
            pltpu.SemaphoreType.DMA((RING,)),
            pltpu.SemaphoreType.DMA((keep + 1,)),
            pltpu.SemaphoreType.DMA((fsdp,)),
            pltpu.SemaphoreType.DMA((7,)),
        ],
        compiler_params=pltpu.CompilerParams(
            collective_id=0, has_side_effects=True, vmem_limit_bytes=VMEM_LIMIT
        ),
        cost_estimate=pl.CostEstimate(
            flops=experts * rows * columns * 30, bytes_accessed=experts * rows * columns * 18, transcendentals=0
        ),
    )(down, gate, up, router, gain)


def rescale(blocks, ready):
    share, inner = blocks[0][0].shape
    width = len(blocks) * inner
    columns = []
    for r in range(0, share, TILE):
        rows = slice(r, min(r + TILE, share))
        parts = [block[rows].astype(jnp.float32) for block, _ in blocks]
        total = sum(jnp.abs(part) for part in parts)
        scale = jnp.sum(total, axis=1, keepdims=True) / width
        inverse = 1.0 / scale
        for (_, at), part in zip(blocks, parts):
            ready[rows, pl.ds(at, inner)] = (part * inverse).astype(jnp.bfloat16)
        columns.append(scale)
    column = jnp.concatenate(columns, axis=0)
    return jnp.broadcast_to(column, (share, 128)).T[0:1]


def finish_kernel(x_ref, copies_ref, *refs):
    readies, scales, router_ref = refs[:3], refs[3:6], refs[6]
    held, ready, router, load_sem, store_sem, router_sem = refs[7:]
    peers, count, _, share, inner = x_ref.shape

    def load(e, kind):
        slot = wrap(e, DEPTH)
        return pltpu.make_async_copy(x_ref.at[:, e, kind], held.at[slot, kind], load_sem.at[slot, kind])

    def store(e, kind):
        slot = wrap(e, DEPTH)
        return pltpu.make_async_copy(ready.at[slot, kind], readies[kind].at[e], store_sem.at[slot, kind])

    for e in range(min(DEPTH, count)):
        for kind in range(3 if e < count - 1 else 2):
            load(e, kind).start()
    enter = pltpu.make_async_copy(copies_ref, router, router_sem.at[0])
    leave = pltpu.make_async_copy(router, router_ref, router_sem.at[1])
    enter.start()

    def settle(e, kind):
        load(e, kind).wait()

        @pl.when(e >= DEPTH)
        def _():
            store(e - DEPTH, kind).wait()

        slot = wrap(e, DEPTH)
        blocks = [(held.at[slot, kind, p], p * inner) for p in range(peers)]
        line = rescale(blocks, ready.at[slot, kind])
        scales[kind][pl.ds(e, 1), :] = line
        store(e, kind).start()

        @pl.when(e + DEPTH < count - (kind == 2))
        def _():
            load(e + DEPTH, kind).start()

    def step_of(e, carry):
        for kind in range(3):
            settle(e, kind)
        return carry

    lax.fori_loop(0, count - 1, step_of, 0)
    settle(count - 1, 0)
    settle(count - 1, 1)
    enter.wait()
    leave.start()
    for kind in range(3):
        end = count - (kind == 2)
        for e in range(max(count - DEPTH, 0), end):
            store(e, kind).wait()
        if kind == 2 and count > DEPTH:
            store(count - 1 - DEPTH, kind).wait()
    leave.wait()


def finish(received, copies, experts):
    peers, count, _, share, inner = received.shape
    width = peers * inner
    hbm = pl.BlockSpec(memory_space=pl.ANY)
    vmem = pl.BlockSpec(memory_space=pltpu.VMEM)
    return pl.pallas_call(
        finish_kernel,
        in_specs=[hbm, hbm],
        out_specs=[hbm] * 3 + [vmem] * 3 + [hbm],
        out_shape=[jax.ShapeDtypeStruct((experts, share, width), jnp.bfloat16)] * 3
        + [jax.ShapeDtypeStruct((experts, share), jnp.float32)] * 3
        + [jax.ShapeDtypeStruct(copies.shape, jnp.bfloat16)],
        scratch_shapes=[
            pltpu.VMEM((DEPTH, 3, peers, share, inner), jnp.bfloat16),
            pltpu.VMEM((DEPTH, 3, share, width), jnp.bfloat16),
            pltpu.VMEM(copies.shape, jnp.bfloat16),
            pltpu.SemaphoreType.DMA((DEPTH, 3)),
            pltpu.SemaphoreType.DMA((DEPTH, 3)),
            pltpu.SemaphoreType.DMA((2,)),
        ],
        compiler_params=pltpu.CompilerParams(vmem_limit_bytes=VMEM_LIMIT),
        cost_estimate=pl.CostEstimate(
            flops=count * share * width * 12, bytes_accessed=count * share * width * 12, transcendentals=0
        ),
    )(received, copies)


def close_kernel(fsdp, first, late_ref, *refs):
    turns = late_turns(fsdp)
    arrived = dict(zip(turns, refs))
    readies, scales = refs[len(turns) + 6 : len(turns) + 9], refs[len(turns) + 9 : len(turns) + 12]
    ready, held, load_sem, store_sem = refs[len(turns) + 12 :]
    _, items, share, inner = late_ref.shape
    me = lax.axis_index("fsdp")
    loads = [pltpu.make_async_copy(scales[kind], held.at[kind], load_sem.at[kind]) for kind in range(3)]
    for load in loads:
        load.start()
    stores = []

    def store(src, dst):
        stores.append(pltpu.make_async_copy(src, dst, store_sem.at[len(stores)]))
        stores[-1].start()

    def column(at):
        return pl.multiple_of(turn(at, me, fsdp, back=True) * inner, inner)

    for kind in range(3):
        for item in range(items):
            e, its = (first - 1, 2) if item == 0 else (first + (item - 1) // 3, (item - 1) % 3)
            if its != kind:
                continue
            blocks = [(late_ref.at[0, item], pl.multiple_of(me * inner, inner)), (late_ref.at[1, item], column(1))]
            blocks += [(ref.at[item], column(at)) for at, ref in arrived.items()]
            line = rescale(blocks, ready.at[item])
            store(ready.at[item], readies[kind].at[e])
            if e <= first and (e < first or kind < 2):
                loads[kind].wait()
            held[kind, e : e + 1, :] = line
        store(held.at[kind], scales[kind])
    for each in stores:
        each.wait()


def close(fsdp, late, arrived, first, carried):
    _, items, share, inner = late.shape
    width = fsdp * inner
    hbm = pl.BlockSpec(memory_space=pl.ANY)
    vmem = pl.BlockSpec(memory_space=pltpu.VMEM)
    return pl.pallas_call(
        functools.partial(close_kernel, fsdp, first),
        in_specs=[vmem] * (len(arrived) + 1) + [hbm] * 6,
        out_specs=[hbm] * 6,
        out_shape=[jax.ShapeDtypeStruct(old.shape, old.dtype) for old in carried],
        input_output_aliases={at + 1 + len(arrived): at for at in range(6)},
        scratch_shapes=[
            pltpu.VMEM((items, share, width), jnp.bfloat16),
            pltpu.VMEM((3,) + carried[3].shape, jnp.float32),
            pltpu.SemaphoreType.DMA((3,)),
            pltpu.SemaphoreType.DMA((items + 3,)),
        ],
        compiler_params=pltpu.CompilerParams(vmem_limit_bytes=FINISH_LIMIT),
        cost_estimate=pl.CostEstimate(
            flops=items * share * width * 4, bytes_accessed=items * share * width * 4, transcendentals=0
        ),
    )(late, *arrived, *carried)


def shards(ep, fsdp, train_gate, train_up, train_down, router_weight, router_gain):
    experts = train_gate.shape[0]
    last = max(experts // 16, 1)
    keep = experts - last
    received, late, copies, *packed = ship(
        ep, fsdp, keep, train_down, train_gate, train_up, router_weight.T, router_gain[None]
    )
    arrived = [
        lax.ppermute(each, "fsdp", [(source, int(turn(at, source, fsdp))) for source in range(fsdp)])
        for at, each in zip(late_turns(fsdp), packed)
    ]
    *done, copies = finish(received, copies, experts)
    ready_down, ready_gate, ready_up, scale_down, scale_gate, scale_up = close(fsdp, late, arrived, keep, done)
    serve_router = copies.reshape(-1, copies.shape[2]).T
    return (
        jnp.swapaxes(ready_gate, 1, 2),
        jnp.swapaxes(ready_up, 1, 2),
        ready_down,
        scale_gate,
        scale_up,
        scale_down,
        serve_router,
    )


def solution(mesh):
    in_specs = (
        P("ep", "fsdp", None),
        P("ep", "fsdp", None),
        P("ep", None, "fsdp"),
        P("fsdp", "ep"),
        P("fsdp"),
    )
    out_specs = (
        P("ep", None, "fsdp"),
        P("ep", None, "fsdp"),
        P("ep", "fsdp", None),
        P("ep", "fsdp"),
        P("ep", "fsdp"),
        P("ep", "fsdp"),
        P(),
    )
    body = functools.partial(shards, mesh.shape["ep"], mesh.shape["fsdp"])
    return jax.shard_map(body, mesh=mesh, in_specs=in_specs, out_specs=out_specs, check_vma=False)
```

```python
import functools

import jax
import jax.numpy as jnp
from jax import lax
from jax.experimental import pallas as pl
from jax.experimental.pallas import tpu as pltpu
from jax.sharding import PartitionSpec as P

VMEM_LIMIT = 60 * 1024 * 1024
FINISH_LIMIT = 24 * 1024 * 1024
TILE = 16
DEPTH = 6
MESH = pl.DeviceIdType.MESH
RING = 6


def turn(at, index, size, back=False):
    if size & (size - 1):
        return (index + (size - at if back else at)) % size
    bits = [1 << bit for bit in range(size.bit_length() - 1)]
    return sum(((index // bit + at // bit) % 2) * bit for bit in bits)


def wrap(e, size):
    return e % size if isinstance(e, int) else lax.rem(e, size)


def late_turns(fsdp):
    near = [at for at in range(2, fsdp) if bin(at // 2).count("1") == 1]
    return near + [at for at in range(2, fsdp) if at not in near]


def ship_kernel(sizes, keep, down_ref, gate_ref, up_ref, router_ref, gain_ref, received_ref, late_ref, copies_ref, *refs):
    ep, fsdp = sizes
    packed = dict(zip(late_turns(fsdp), refs))
    down_in, gate_in, up_in, ring, weight, gain, strip = refs[len(packed) : len(packed) + 7]
    load_sem, send_sem, recv_sem, piece_sem, router_sem = refs[len(packed) + 7 :]
    row, me = lax.axis_index("ep"), lax.axis_index("fsdp")
    experts = down_ref.shape[0]
    sources = ((down_ref, down_in), (gate_ref, gate_in), (up_ref, up_in))

    def load(e, kind):
        source, held = sources[kind]
        slot = wrap(e, 2)
        return pltpu.make_async_copy(source.at[e], held.at[slot], load_sem.at[slot, kind])

    def pack(e, kind):
        block = sources[kind][1][wrap(e, 2)].astype(jnp.bfloat16)
        if kind:
            block = block.T
        ring[wrap(e, RING), :, kind] = block.reshape(fsdp, *ring.shape[3:])

    def sent(e):
        slot = wrap(e, RING)
        return pltpu.make_async_copy(ring.at[slot], received_ref.at[:, 0], send_sem.at[slot])

    order = [lax.rem(me + step, fsdp) for step in range(1, fsdp + 1)]

    def ship(src, dst, slot, e, peer):
        return pltpu.make_async_remote_copy(
            src_ref=src,
            dst_ref=dst,
            send_sem=send_sem.at[slot],
            recv_sem=recv_sem.at[e],
            device_id={"fsdp": peer},
            device_id_type=MESH,
        )

    def send(e):
        slot = wrap(e, RING)
        for peer in order[:-1]:
            ship(ring.at[slot, peer], received_ref.at[me, e], slot, e, peer).start()
        pltpu.make_async_copy(ring.at[slot, me], received_ref.at[me, e], send_sem.at[slot]).start()

    def piece(at, p):
        share = ring.shape[3]
        rows = pl.ds(pl.multiple_of(p * share, share), share)
        return pltpu.make_async_copy(down_ref.at[0, rows], down_in.at[0, rows], piece_sem.at[at])

    router = [
        pltpu.make_async_copy(src, dst, router_sem.at[at])
        for at, (src, dst) in enumerate(((router_ref, weight), (gain_ref, gain)))
    ]

    barrier = pltpu.get_barrier_semaphore()
    for step in range(1, fsdp):
        pl.semaphore_signal(barrier, device_id={"fsdp": lax.rem(me + step, fsdp)}, device_id_type=MESH)
    for step in range(1, ep):
        pl.semaphore_signal(barrier, device_id={"ep": lax.rem(row + step, ep)}, device_id_type=MESH)
    for at, p in enumerate(order):
        piece(at, p).start()
    pl.semaphore_wait(barrier, fsdp + ep - 2)

    for at, p in enumerate(order):
        piece(at, p).wait()
        share = ring.shape[3]
        rows = pl.ds(pl.multiple_of(p * share, share), share)
        ring[0, p, 0] = down_in[0, rows].astype(jnp.bfloat16)
        if at < fsdp - 1:
            ship(ring.at[0, p, 0], received_ref.at[me, 0, 0], 0, 0, p).start()
        if at == fsdp // 2:
            load(0, 1).start()
    load(0, 2).start()
    for copy in router:
        copy.start()
    for kind in range(3):
        load(1, kind).start()
    for kind in (1, 2):
        load(0, kind).wait()
        pack(0, kind)
        for peer in order[:-1]:
            ship(ring.at[0, peer, kind], received_ref.at[me, 0, kind], 0, 0, peer).start()
    pltpu.make_async_copy(ring.at[0, me], received_ref.at[me, 0], send_sem.at[0]).start()
    if experts > 2:
        for kind in range(3):
            load(2, kind).start()

    def prepare(e, kind):
        load(e, kind).wait()
        if kind == 0:

            @pl.when(e >= RING)
            def _():
                sent(e - RING).wait()

        pack(e, kind)

        @pl.when(e + 2 < experts)
        def _():
            load(e + 2, kind).start()

    def step_of(e, carry):
        for kind in range(3):
            prepare(e, kind)
        send(e)
        return carry

    def set_by(e, kind, item):
        slot = e % RING
        for at, ref in packed.items():
            peer = turn(at, me, fsdp)
            pltpu.make_async_copy(ring.at[slot, peer, kind], ref.at[item], send_sem.at[slot]).start()
        peer = turn(1, me, fsdp)
        ship(ring.at[slot, peer, kind], late_ref.at[1, item], slot, keep, peer).start()
        pltpu.make_async_copy(ring.at[slot, me, kind], late_ref.at[0, item], send_sem.at[slot]).start()

    first = min(RING, keep - 1)
    lax.fori_loop(1, first, step_of, 0)

    width = weight.shape[1]
    mine = strip.at[:, pl.ds(pl.multiple_of(me * width, width), width)]
    for copy in router:
        copy.wait()
    mine[...] = (weight[...] * gain[...]).astype(jnp.bfloat16)
    for peer in order[:-1]:
        pltpu.make_async_remote_copy(
            src_ref=mine,
            dst_ref=mine,
            send_sem=router_sem.at[2],
            recv_sem=router_sem.at[3],
            device_id={"fsdp": peer},
            device_id_type=MESH,
        ).start()
    lax.fori_loop(first, keep - 1, step_of, 0)
    e, slot = keep - 1, (keep - 1) % RING
    prepare(e, 0)
    prepare(e, 1)
    two = pl.ds(0, 2)
    for peer in order[:-1]:
        ship(ring.at[slot, peer, two], received_ref.at[me, e, two], slot, e, peer).start()
    pltpu.make_async_copy(ring.at[slot, me, two], received_ref.at[me, e, two], send_sem.at[slot]).start()
    prepare(e, 2)
    set_by(e, 2, 0)
    others = strip.at[:, pl.ds(0, (fsdp - 1) * width)]
    pltpu.make_async_copy(others, others, router_sem.at[2]).wait()
    pltpu.make_async_copy(others, others, router_sem.at[3]).wait()
    for step in range(1, ep):
        pltpu.make_async_remote_copy(
            src_ref=strip,
            dst_ref=copies_ref.at[row],
            send_sem=router_sem.at[4],
            recv_sem=router_sem.at[5],
            device_id={"ep": lax.rem(row + step, ep)},
            device_id_type=MESH,
        ).start()
    own = pltpu.make_async_copy(strip, copies_ref.at[row], router_sem.at[6])
    own.start()
    for e in range(keep, experts):
        for kind in range(3):
            prepare(e, kind)
            set_by(e, kind, 1 + 3 * (e - keep) + kind)

    def settle(e, carry):
        sent(e).wait()
        return carry

    lax.fori_loop(max(experts - RING, 0), experts, settle, 0)

    def arrive(e, carry):
        blocks = received_ref.at[pl.ds(0, fsdp - 1), e]
        pltpu.make_async_copy(blocks, blocks, recv_sem.at[e]).wait()
        return carry

    lax.fori_loop(0, keep - 1, arrive, 0)
    blocks = received_ref.at[pl.ds(0, fsdp - 1), 0, two]
    pltpu.make_async_copy(blocks, blocks, recv_sem.at[keep - 1]).wait()
    pltpu.make_async_copy(late_ref.at[1], late_ref.at[1], recv_sem.at[keep]).wait()
    others = copies_ref.at[pl.ds(0, ep - 1)]
    pltpu.make_async_copy(others, others, router_sem.at[4]).wait()
    pltpu.make_async_copy(others, others, router_sem.at[5]).wait()
    own.wait()


def ship(ep, fsdp, keep, down, gate, up, router, gain):
    experts, rows, columns = gate.shape
    share = columns // fsdp
    late = 1 + 3 * (experts - keep)
    hbm = pl.BlockSpec(memory_space=pl.ANY)
    return pl.pallas_call(
        functools.partial(ship_kernel, (ep, fsdp), keep),
        in_specs=[hbm] * 5,
        out_specs=[hbm] * (fsdp + 1),
        out_shape=[
            jax.ShapeDtypeStruct((fsdp, keep, 3, share, rows), jnp.bfloat16),
            jax.ShapeDtypeStruct((2, late, share, rows), jnp.bfloat16),
            jax.ShapeDtypeStruct((ep, router.shape[0], fsdp * router.shape[1]), jnp.bfloat16),
        ]
        + [jax.ShapeDtypeStruct((late, share, rows), jnp.bfloat16)] * (fsdp - 2),
        scratch_shapes=[
            pltpu.VMEM((2, columns, rows), jnp.float32),
            pltpu.VMEM((2, rows, columns), jnp.float32),
            pltpu.VMEM((2, rows, columns), jnp.float32),
            pltpu.VMEM((RING, fsdp, 3, share, rows), jnp.bfloat16),
            pltpu.VMEM(router.shape, jnp.float32),
            pltpu.VMEM(gain.shape, jnp.float32),
            pltpu.VMEM((router.shape[0], fsdp * router.shape[1]), jnp.bfloat16),
            pltpu.SemaphoreType.DMA((2, 3)),
            pltpu.SemaphoreType.DMA((RING,)),
            pltpu.SemaphoreType.DMA((keep + 1,)),
            pltpu.SemaphoreType.DMA((fsdp,)),
            pltpu.SemaphoreType.DMA((7,)),
        ],
        compiler_params=pltpu.CompilerParams(
            collective_id=0, has_side_effects=True, vmem_limit_bytes=VMEM_LIMIT
        ),
        cost_estimate=pl.CostEstimate(
            flops=experts * rows * columns * 30, bytes_accessed=experts * rows * columns * 18, transcendentals=0
        ),
    )(down, gate, up, router, gain)


def rescale(blocks, ready):
    share, inner = blocks[0][0].shape
    width = len(blocks) * inner
    columns = []
    for r in range(0, share, TILE):
        rows = slice(r, min(r + TILE, share))
        parts = [block[rows].astype(jnp.float32) for block, _ in blocks]
        total = sum(jnp.abs(part) for part in parts)
        scale = jnp.sum(total, axis=1, keepdims=True) / width
        inverse = 1.0 / scale
        for (_, at), part in zip(blocks, parts):
            ready[rows, pl.ds(at, inner)] = (part * inverse).astype(jnp.bfloat16)
        columns.append(scale)
    column = jnp.concatenate(columns, axis=0)
    return jnp.broadcast_to(column, (share, 128)).T[0:1]


def finish_kernel(x_ref, copies_ref, *refs):
    readies, scales, router_ref = refs[:3], refs[3:6], refs[6]
    held, ready, router, load_sem, store_sem, router_sem = refs[7:]
    peers, count, _, share, inner = x_ref.shape

    def load(e, kind):
        slot = wrap(e, DEPTH)
        return pltpu.make_async_copy(x_ref.at[:, e, kind], held.at[slot, kind], load_sem.at[slot, kind])

    def store(e, kind):
        slot = wrap(e, DEPTH)
        return pltpu.make_async_copy(ready.at[slot, kind], readies[kind].at[e], store_sem.at[slot, kind])

    for e in range(min(DEPTH, count)):
        for kind in range(3 if e < count - 1 else 2):
            load(e, kind).start()
    enter = pltpu.make_async_copy(copies_ref, router, router_sem.at[0])
    leave = pltpu.make_async_copy(router, router_ref, router_sem.at[1])
    enter.start()

    def settle(e, kind):
        load(e, kind).wait()

        @pl.when(e >= DEPTH)
        def _():
            store(e - DEPTH, kind).wait()

        slot = wrap(e, DEPTH)
        blocks = [(held.at[slot, kind, p], p * inner) for p in range(peers)]
        line = rescale(blocks, ready.at[slot, kind])
        scales[kind][pl.ds(e, 1), :] = line
        store(e, kind).start()

        @pl.when(e + DEPTH < count - (kind == 2))
        def _():
            load(e + DEPTH, kind).start()

    def step_of(e, carry):
        for kind in range(3):
            settle(e, kind)
        return carry

    lax.fori_loop(0, count - 1, step_of, 0)
    settle(count - 1, 0)
    settle(count - 1, 1)
    enter.wait()
    leave.start()
    for kind in range(3):
        end = count - (kind == 2)
        for e in range(max(count - DEPTH, 0), end):
            store(e, kind).wait()
        if kind == 2 and count > DEPTH:
            store(count - 1 - DEPTH, kind).wait()
    leave.wait()


def finish(received, copies, experts):
    peers, count, _, share, inner = received.shape
    width = peers * inner
    hbm = pl.BlockSpec(memory_space=pl.ANY)
    vmem = pl.BlockSpec(memory_space=pltpu.VMEM)
    return pl.pallas_call(
        finish_kernel,
        in_specs=[hbm, hbm],
        out_specs=[hbm] * 3 + [vmem] * 3 + [hbm],
        out_shape=[jax.ShapeDtypeStruct((experts, share, width), jnp.bfloat16)] * 3
        + [jax.ShapeDtypeStruct((experts, share), jnp.float32)] * 3
        + [jax.ShapeDtypeStruct(copies.shape, jnp.bfloat16)],
        scratch_shapes=[
            pltpu.VMEM((DEPTH, 3, peers, share, inner), jnp.bfloat16),
            pltpu.VMEM((DEPTH, 3, share, width), jnp.bfloat16),
            pltpu.VMEM(copies.shape, jnp.bfloat16),
            pltpu.SemaphoreType.DMA((DEPTH, 3)),
            pltpu.SemaphoreType.DMA((DEPTH, 3)),
            pltpu.SemaphoreType.DMA((2,)),
        ],
        compiler_params=pltpu.CompilerParams(vmem_limit_bytes=VMEM_LIMIT),
        cost_estimate=pl.CostEstimate(
            flops=count * share * width * 12, bytes_accessed=count * share * width * 12, transcendentals=0
        ),
    )(received, copies)


def close_kernel(fsdp, first, late_ref, *refs):
    turns = late_turns(fsdp)
    arrived = dict(zip(turns, refs))
    readies, scales = refs[len(turns) + 6 : len(turns) + 9], refs[len(turns) + 9 : len(turns) + 12]
    ready, held, load_sem, store_sem = refs[len(turns) + 12 :]
    _, items, share, inner = late_ref.shape
    me = lax.axis_index("fsdp")
    loads = [pltpu.make_async_copy(scales[kind], held.at[kind], load_sem.at[kind]) for kind in range(3)]
    for load in loads:
        load.start()
    stores = []

    def store(src, dst):
        stores.append(pltpu.make_async_copy(src, dst, store_sem.at[len(stores)]))
        stores[-1].start()

    def column(at):
        return pl.multiple_of(turn(at, me, fsdp, back=True) * inner, inner)

    lines = []
    for item in range(items):
        e, kind = (first - 1, 2) if item == 0 else (first + (item - 1) // 3, (item - 1) % 3)
        blocks = [(late_ref.at[0, item], pl.multiple_of(me * inner, inner)), (late_ref.at[1, item], column(1))]
        blocks += [(ref.at[item], column(at)) for at, ref in arrived.items()]
        lines.append((kind, e, rescale(blocks, ready.at[item])))
        store(ready.at[item], readies[kind].at[e])
    for load in loads:
        load.wait()
    for kind, e, line in lines:
        held[kind, e : e + 1, :] = line
    for kind in range(3):
        store(held.at[kind], scales[kind])
    for each in stores:
        each.wait()


def close(fsdp, late, arrived, first, carried):
    _, items, share, inner = late.shape
    width = fsdp * inner
    hbm = pl.BlockSpec(memory_space=pl.ANY)
    vmem = pl.BlockSpec(memory_space=pltpu.VMEM)
    return pl.pallas_call(
        functools.partial(close_kernel, fsdp, first),
        in_specs=[vmem] * (len(arrived) + 1) + [hbm] * 6,
        out_specs=[hbm] * 6,
        out_shape=[jax.ShapeDtypeStruct(old.shape, old.dtype) for old in carried],
        input_output_aliases={at + 1 + len(arrived): at for at in range(6)},
        scratch_shapes=[
            pltpu.VMEM((items, share, width), jnp.bfloat16),
            pltpu.VMEM((3,) + carried[3].shape, jnp.float32),
            pltpu.SemaphoreType.DMA((3,)),
            pltpu.SemaphoreType.DMA((items + 3,)),
        ],
        compiler_params=pltpu.CompilerParams(vmem_limit_bytes=FINISH_LIMIT),
        cost_estimate=pl.CostEstimate(
            flops=items * share * width * 4, bytes_accessed=items * share * width * 4, transcendentals=0
        ),
    )(late, *arrived, *carried)


def shards(ep, fsdp, train_gate, train_up, train_down, router_weight, router_gain):
    experts = train_gate.shape[0]
    last = max(experts // 16, 1)
    keep = experts - last
    received, late, copies, *packed = ship(
        ep, fsdp, keep, train_down, train_gate, train_up, router_weight.T, router_gain[None]
    )
    arrived = [
        lax.ppermute(each, "fsdp", [(source, int(turn(at, source, fsdp))) for source in range(fsdp)])
        for at, each in zip(late_turns(fsdp), packed)
    ]
    *done, copies = finish(received, copies, experts)
    ready_down, ready_gate, ready_up, scale_down, scale_gate, scale_up = close(fsdp, late, arrived, keep, done)
    serve_router = copies.reshape(-1, copies.shape[2]).T
    return (
        jnp.swapaxes(ready_gate, 1, 2),
        jnp.swapaxes(ready_up, 1, 2),
        ready_down,
        scale_gate,
        scale_up,
        scale_down,
        serve_router,
    )


def solution(mesh):
    in_specs = (
        P("ep", "fsdp", None),
        P("ep", "fsdp", None),
        P("ep", None, "fsdp"),
        P("fsdp", "ep"),
        P("fsdp"),
    )
    out_specs = (
        P("ep", None, "fsdp"),
        P("ep", None, "fsdp"),
        P("ep", "fsdp", None),
        P("ep", "fsdp"),
        P("ep", "fsdp"),
        P("ep", "fsdp"),
        P(),
    )
    body = functools.partial(shards, mesh.shape["ep"], mesh.shape["fsdp"])
    return jax.shard_map(body, mesh=mesh, in_specs=in_specs, out_specs=out_specs, check_vma=False)
```

```python
import functools

import jax
import jax.numpy as jnp
from jax import lax
from jax.experimental import pallas as pl
from jax.experimental.pallas import tpu as pltpu
from jax.sharding import PartitionSpec as P

VMEM_LIMIT = 60 * 1024 * 1024
FINISH_LIMIT = 24 * 1024 * 1024
TILE = 16
DEPTH = 6
MESH = pl.DeviceIdType.MESH
RING = 6


def turn(at, index, size, back=False):
    if size & (size - 1):
        return (index + (size - at if back else at)) % size
    bits = [1 << bit for bit in range(size.bit_length() - 1)]
    return sum(((index // bit + at // bit) % 2) * bit for bit in bits)


def wrap(e, size):
    return e % size if isinstance(e, int) else lax.rem(e, size)


def late_turns(fsdp):
    near = [at for at in range(2, fsdp) if bin(at // 2).count("1") == 1]
    return near + [at for at in range(2, fsdp) if at not in near]


def ship_kernel(sizes, keep, down_ref, gate_ref, up_ref, router_ref, gain_ref, received_ref, late_ref, copies_ref, *refs):
    ep, fsdp = sizes
    packed = dict(zip(late_turns(fsdp), refs))
    down_in, gate_in, up_in, ring, weight, gain, strip = refs[len(packed) : len(packed) + 7]
    load_sem, send_sem, recv_sem, piece_sem, router_sem = refs[len(packed) + 7 :]
    row, me = lax.axis_index("ep"), lax.axis_index("fsdp")
    experts = down_ref.shape[0]
    sources = ((down_ref, down_in), (gate_ref, gate_in), (up_ref, up_in))

    def load(e, kind):
        source, held = sources[kind]
        slot = wrap(e, 2)
        return pltpu.make_async_copy(source.at[e], held.at[slot], load_sem.at[slot, kind])

    def pack(e, kind):
        block = sources[kind][1][wrap(e, 2)].astype(jnp.bfloat16)
        if kind:
            block = block.T
        ring[wrap(e, RING), :, kind] = block.reshape(fsdp, *ring.shape[3:])

    def sent(e):
        slot = wrap(e, RING)
        return pltpu.make_async_copy(ring.at[slot], received_ref.at[:, 0], send_sem.at[slot])

    order = [turn(at, me, fsdp) for at in late_turns(fsdp) + [1, 0]]

    def ship(src, dst, slot, e, peer):
        return pltpu.make_async_remote_copy(
            src_ref=src,
            dst_ref=dst,
            send_sem=send_sem.at[slot],
            recv_sem=recv_sem.at[e],
            device_id={"fsdp": peer},
            device_id_type=MESH,
        )

    def send(e):
        slot = wrap(e, RING)
        for peer in order[:-1]:
            ship(ring.at[slot, peer], received_ref.at[me, e], slot, e, peer).start()
        pltpu.make_async_copy(ring.at[slot, me], received_ref.at[me, e], send_sem.at[slot]).start()

    def piece(at, p):
        share = ring.shape[3]
        rows = pl.ds(pl.multiple_of(p * share, share), share)
        return pltpu.make_async_copy(down_ref.at[0, rows], down_in.at[0, rows], piece_sem.at[at])

    router = [
        pltpu.make_async_copy(src, dst, router_sem.at[at])
        for at, (src, dst) in enumerate(((router_ref, weight), (gain_ref, gain)))
    ]

    barrier = pltpu.get_barrier_semaphore()
    for step in range(1, fsdp):
        pl.semaphore_signal(barrier, device_id={"fsdp": lax.rem(me + step, fsdp)}, device_id_type=MESH)
    for step in range(1, ep):
        pl.semaphore_signal(barrier, device_id={"ep": lax.rem(row + step, ep)}, device_id_type=MESH)
    for at, p in enumerate(order):
        piece(at, p).start()
    pl.semaphore_wait(barrier, fsdp + ep - 2)

    for at, p in enumerate(order):
        piece(at, p).wait()
        share = ring.shape[3]
        rows = pl.ds(pl.multiple_of(p * share, share), share)
        ring[0, p, 0] = down_in[0, rows].astype(jnp.bfloat16)
        if at < fsdp - 1:
            ship(ring.at[0, p, 0], received_ref.at[me, 0, 0], 0, 0, p).start()
        if at == fsdp // 2:
            load(0, 1).start()
    load(0, 2).start()
    for copy in router:
        copy.start()
    for kind in range(3):
        load(1, kind).start()
    for kind in (1, 2):
        load(0, kind).wait()
        pack(0, kind)
        for peer in order[:-1]:
            ship(ring.at[0, peer, kind], received_ref.at[me, 0, kind], 0, 0, peer).start()
    pltpu.make_async_copy(ring.at[0, me], received_ref.at[me, 0], send_sem.at[0]).start()
    if experts > 2:
        for kind in range(3):
            load(2, kind).start()

    def prepare(e, kind):
        load(e, kind).wait()
        if kind == 0:

            @pl.when(e >= RING)
            def _():
                sent(e - RING).wait()

        pack(e, kind)

        @pl.when(e + 2 < experts)
        def _():
            load(e + 2, kind).start()

    def step_of(e, carry):
        for kind in range(3):
            prepare(e, kind)
        send(e)
        return carry

    def set_by(e, kind, item):
        slot = e % RING
        for at, ref in packed.items():
            peer = turn(at, me, fsdp)
            pltpu.make_async_copy(ring.at[slot, peer, kind], ref.at[item], send_sem.at[slot]).start()
        peer = turn(1, me, fsdp)
        ship(ring.at[slot, peer, kind], late_ref.at[1, item], slot, keep, peer).start()
        pltpu.make_async_copy(ring.at[slot, me, kind], late_ref.at[0, item], send_sem.at[slot]).start()

    first = min(RING, keep - 1)
    lax.fori_loop(1, first, step_of, 0)

    width = weight.shape[1]
    mine = strip.at[:, pl.ds(pl.multiple_of(me * width, width), width)]
    for copy in router:
        copy.wait()
    mine[...] = (weight[...] * gain[...]).astype(jnp.bfloat16)
    for peer in order[:-1]:
        pltpu.make_async_remote_copy(
            src_ref=mine,
            dst_ref=mine,
            send_sem=router_sem.at[2],
            recv_sem=router_sem.at[3],
            device_id={"fsdp": peer},
            device_id_type=MESH,
        ).start()
    lax.fori_loop(first, keep - 1, step_of, 0)
    e, slot = keep - 1, (keep - 1) % RING
    prepare(e, 0)
    prepare(e, 1)
    two = pl.ds(0, 2)
    for peer in order[:-1]:
        ship(ring.at[slot, peer, two], received_ref.at[me, e, two], slot, e, peer).start()
    pltpu.make_async_copy(ring.at[slot, me, two], received_ref.at[me, e, two], send_sem.at[slot]).start()
    prepare(e, 2)
    set_by(e, 2, 0)
    others = strip.at[:, pl.ds(0, (fsdp - 1) * width)]
    pltpu.make_async_copy(others, others, router_sem.at[2]).wait()
    pltpu.make_async_copy(others, others, router_sem.at[3]).wait()
    for step in range(1, ep):
        pltpu.make_async_remote_copy(
            src_ref=strip,
            dst_ref=copies_ref.at[row],
            send_sem=router_sem.at[4],
            recv_sem=router_sem.at[5],
            device_id={"ep": lax.rem(row + step, ep)},
            device_id_type=MESH,
        ).start()
    own = pltpu.make_async_copy(strip, copies_ref.at[row], router_sem.at[6])
    own.start()
    for e in range(keep, experts):
        for kind in range(3):
            prepare(e, kind)
            set_by(e, kind, 1 + 3 * (e - keep) + kind)

    def settle(e, carry):
        sent(e).wait()
        return carry

    lax.fori_loop(max(experts - RING, 0), experts, settle, 0)

    def arrive(e, carry):
        blocks = received_ref.at[pl.ds(0, fsdp - 1), e]
        pltpu.make_async_copy(blocks, blocks, recv_sem.at[e]).wait()
        return carry

    lax.fori_loop(0, keep - 1, arrive, 0)
    blocks = received_ref.at[pl.ds(0, fsdp - 1), 0, two]
    pltpu.make_async_copy(blocks, blocks, recv_sem.at[keep - 1]).wait()
    pltpu.make_async_copy(late_ref.at[1], late_ref.at[1], recv_sem.at[keep]).wait()
    others = copies_ref.at[pl.ds(0, ep - 1)]
    pltpu.make_async_copy(others, others, router_sem.at[4]).wait()
    pltpu.make_async_copy(others, others, router_sem.at[5]).wait()
    own.wait()


def ship(ep, fsdp, keep, down, gate, up, router, gain):
    experts, rows, columns = gate.shape
    share = columns // fsdp
    late = 1 + 3 * (experts - keep)
    hbm = pl.BlockSpec(memory_space=pl.ANY)
    return pl.pallas_call(
        functools.partial(ship_kernel, (ep, fsdp), keep),
        in_specs=[hbm] * 5,
        out_specs=[hbm] * (fsdp + 1),
        out_shape=[
            jax.ShapeDtypeStruct((fsdp, keep, 3, share, rows), jnp.bfloat16),
            jax.ShapeDtypeStruct((2, late, share, rows), jnp.bfloat16),
            jax.ShapeDtypeStruct((ep, router.shape[0], fsdp * router.shape[1]), jnp.bfloat16),
        ]
        + [jax.ShapeDtypeStruct((late, share, rows), jnp.bfloat16)] * (fsdp - 2),
        scratch_shapes=[
            pltpu.VMEM((2, columns, rows), jnp.float32),
            pltpu.VMEM((2, rows, columns), jnp.float32),
            pltpu.VMEM((2, rows, columns), jnp.float32),
            pltpu.VMEM((RING, fsdp, 3, share, rows), jnp.bfloat16),
            pltpu.VMEM(router.shape, jnp.float32),
            pltpu.VMEM(gain.shape, jnp.float32),
            pltpu.VMEM((router.shape[0], fsdp * router.shape[1]), jnp.bfloat16),
            pltpu.SemaphoreType.DMA((2, 3)),
            pltpu.SemaphoreType.DMA((RING,)),
            pltpu.SemaphoreType.DMA((keep + 1,)),
            pltpu.SemaphoreType.DMA((fsdp,)),
            pltpu.SemaphoreType.DMA((7,)),
        ],
        compiler_params=pltpu.CompilerParams(
            collective_id=0, has_side_effects=True, vmem_limit_bytes=VMEM_LIMIT
        ),
        cost_estimate=pl.CostEstimate(
            flops=experts * rows * columns * 30, bytes_accessed=experts * rows * columns * 18, transcendentals=0
        ),
    )(down, gate, up, router, gain)


def rescale(blocks, ready):
    share, inner = blocks[0][0].shape
    width = len(blocks) * inner
    columns = []
    for r in range(0, share, TILE):
        rows = slice(r, min(r + TILE, share))
        parts = [block[rows].astype(jnp.float32) for block, _ in blocks]
        total = sum(jnp.abs(part) for part in parts)
        scale = jnp.sum(total, axis=1, keepdims=True) / width
        inverse = 1.0 / scale
        for (_, at), part in zip(blocks, parts):
            ready[rows, pl.ds(at, inner)] = (part * inverse).astype(jnp.bfloat16)
        columns.append(scale)
    column = jnp.concatenate(columns, axis=0)
    return jnp.broadcast_to(column, (share, 128)).T[0:1]


def finish_kernel(x_ref, copies_ref, *refs):
    readies, scales, router_ref = refs[:3], refs[3:6], refs[6]
    held, ready, router, load_sem, store_sem, router_sem = refs[7:]
    peers, count, _, share, inner = x_ref.shape

    def load(e, kind):
        slot = wrap(e, DEPTH)
        return pltpu.make_async_copy(x_ref.at[:, e, kind], held.at[slot, kind], load_sem.at[slot, kind])

    def store(e, kind):
        slot = wrap(e, DEPTH)
        return pltpu.make_async_copy(ready.at[slot, kind], readies[kind].at[e], store_sem.at[slot, kind])

    for e in range(min(DEPTH, count)):
        for kind in range(3 if e < count - 1 else 2):
            load(e, kind).start()
    enter = pltpu.make_async_copy(copies_ref, router, router_sem.at[0])
    leave = pltpu.make_async_copy(router, router_ref, router_sem.at[1])
    enter.start()

    def settle(e, kind):
        load(e, kind).wait()

        @pl.when(e >= DEPTH)
        def _():
            store(e - DEPTH, kind).wait()

        slot = wrap(e, DEPTH)
        blocks = [(held.at[slot, kind, p], p * inner) for p in range(peers)]
        line = rescale(blocks, ready.at[slot, kind])
        scales[kind][pl.ds(e, 1), :] = line
        store(e, kind).start()

        @pl.when(e + DEPTH < count - (kind == 2))
        def _():
            load(e + DEPTH, kind).start()

    def step_of(e, carry):
        for kind in range(3):
            settle(e, kind)
        return carry

    lax.fori_loop(0, count - 1, step_of, 0)
    settle(count - 1, 0)
    settle(count - 1, 1)
    enter.wait()
    leave.start()
    for kind in range(3):
        end = count - (kind == 2)
        for e in range(max(count - DEPTH, 0), end):
            store(e, kind).wait()
        if kind == 2 and count > DEPTH:
            store(count - 1 - DEPTH, kind).wait()
    leave.wait()


def finish(received, copies, experts):
    peers, count, _, share, inner = received.shape
    width = peers * inner
    hbm = pl.BlockSpec(memory_space=pl.ANY)
    vmem = pl.BlockSpec(memory_space=pltpu.VMEM)
    return pl.pallas_call(
        finish_kernel,
        in_specs=[hbm, hbm],
        out_specs=[hbm] * 3 + [vmem] * 3 + [hbm],
        out_shape=[jax.ShapeDtypeStruct((experts, share, width), jnp.bfloat16)] * 3
        + [jax.ShapeDtypeStruct((experts, share), jnp.float32)] * 3
        + [jax.ShapeDtypeStruct(copies.shape, jnp.bfloat16)],
        scratch_shapes=[
            pltpu.VMEM((DEPTH, 3, peers, share, inner), jnp.bfloat16),
            pltpu.VMEM((DEPTH, 3, share, width), jnp.bfloat16),
            pltpu.VMEM(copies.shape, jnp.bfloat16),
            pltpu.SemaphoreType.DMA((DEPTH, 3)),
            pltpu.SemaphoreType.DMA((DEPTH, 3)),
            pltpu.SemaphoreType.DMA((2,)),
        ],
        compiler_params=pltpu.CompilerParams(vmem_limit_bytes=VMEM_LIMIT),
        cost_estimate=pl.CostEstimate(
            flops=count * share * width * 12, bytes_accessed=count * share * width * 12, transcendentals=0
        ),
    )(received, copies)


def close_kernel(fsdp, first, late_ref, *refs):
    turns = late_turns(fsdp)
    arrived = dict(zip(turns, refs))
    readies, scales = refs[len(turns) + 6 : len(turns) + 9], refs[len(turns) + 9 : len(turns) + 12]
    ready, held, load_sem, store_sem = refs[len(turns) + 12 :]
    _, items, share, inner = late_ref.shape
    me = lax.axis_index("fsdp")
    loads = [pltpu.make_async_copy(scales[kind], held.at[kind], load_sem.at[kind]) for kind in range(3)]
    for load in loads:
        load.start()
    stores = []

    def store(src, dst):
        stores.append(pltpu.make_async_copy(src, dst, store_sem.at[len(stores)]))
        stores[-1].start()

    def column(at):
        return pl.multiple_of(turn(at, me, fsdp, back=True) * inner, inner)

    lines = []
    for item in range(items):
        e, kind = (first - 1, 2) if item == 0 else (first + (item - 1) // 3, (item - 1) % 3)
        blocks = [(late_ref.at[0, item], pl.multiple_of(me * inner, inner)), (late_ref.at[1, item], column(1))]
        blocks += [(ref.at[item], column(at)) for at, ref in arrived.items()]
        lines.append((kind, e, rescale(blocks, ready.at[item])))
        store(ready.at[item], readies[kind].at[e])
    for load in loads:
        load.wait()
    for kind, e, line in lines:
        held[kind, e : e + 1, :] = line
    for kind in range(3):
        store(held.at[kind], scales[kind])
    for each in stores:
        each.wait()


def close(fsdp, late, arrived, first, carried):
    _, items, share, inner = late.shape
    width = fsdp * inner
    hbm = pl.BlockSpec(memory_space=pl.ANY)
    vmem = pl.BlockSpec(memory_space=pltpu.VMEM)
    return pl.pallas_call(
        functools.partial(close_kernel, fsdp, first),
        in_specs=[vmem] * (len(arrived) + 1) + [hbm] * 6,
        out_specs=[hbm] * 6,
        out_shape=[jax.ShapeDtypeStruct(old.shape, old.dtype) for old in carried],
        input_output_aliases={at + 1 + len(arrived): at for at in range(6)},
        scratch_shapes=[
            pltpu.VMEM((items, share, width), jnp.bfloat16),
            pltpu.VMEM((3,) + carried[3].shape, jnp.float32),
            pltpu.SemaphoreType.DMA((3,)),
            pltpu.SemaphoreType.DMA((items + 3,)),
        ],
        compiler_params=pltpu.CompilerParams(vmem_limit_bytes=FINISH_LIMIT),
        cost_estimate=pl.CostEstimate(
            flops=items * share * width * 4, bytes_accessed=items * share * width * 4, transcendentals=0
        ),
    )(late, *arrived, *carried)


def shards(ep, fsdp, train_gate, train_up, train_down, router_weight, router_gain):
    experts = train_gate.shape[0]
    last = max(experts // 16, 1)
    keep = experts - last
    received, late, copies, *packed = ship(
        ep, fsdp, keep, train_down, train_gate, train_up, router_weight.T, router_gain[None]
    )
    arrived = [
        lax.ppermute(each, "fsdp", [(source, int(turn(at, source, fsdp))) for source in range(fsdp)])
        for at, each in zip(late_turns(fsdp), packed)
    ]
    *done, copies = finish(received, copies, experts)
    ready_down, ready_gate, ready_up, scale_down, scale_gate, scale_up = close(fsdp, late, arrived, keep, done)
    serve_router = copies.reshape(-1, copies.shape[2]).T
    return (
        jnp.swapaxes(ready_gate, 1, 2),
        jnp.swapaxes(ready_up, 1, 2),
        ready_down,
        scale_gate,
        scale_up,
        scale_down,
        serve_router,
    )


def solution(mesh):
    in_specs = (
        P("ep", "fsdp", None),
        P("ep", "fsdp", None),
        P("ep", None, "fsdp"),
        P("fsdp", "ep"),
        P("fsdp"),
    )
    out_specs = (
        P("ep", None, "fsdp"),
        P("ep", None, "fsdp"),
        P("ep", "fsdp", None),
        P("ep", "fsdp"),
        P("ep", "fsdp"),
        P("ep", "fsdp"),
        P(),
    )
    body = functools.partial(shards, mesh.shape["ep"], mesh.shape["fsdp"])
    return jax.shard_map(body, mesh=mesh, in_specs=in_specs, out_specs=out_specs, check_vma=False)
```
